256 devices in a mesh: ops: 64 (over x, z, core), sec: 4 (over y).
Axes of the slice: x: 4, y: 4, z: 8, core: 2. Of those that a mesh axis runs over, the one named last changes fastest.
Arguments:
- operators: bfloat16 [128, 8, 768, 768], P('ops', 'sec'), may hold values from -6 to 6
- basis: bfloat16 [8, 768, 768], P('sec'), may hold values from -0.21875 to 0.21875
- shift: int32 [128], replicated, may hold values from -1 to 1
- dest: int32 [128], replicated, may hold values from 0 to 127, each once
- sector_sizes: int32 [8], replicated, may hold values from 384 to 768
Outputs:
- renormalized: bfloat16 [128, 8, 768, 768], P('ops', 'sec')
The draws below stay inside these ranges and needn't reach their ends.
Inputs may be any that keep to these rules, and one draw needn't show every extreme that they name: `shift`: each pair's offset is -1, 0 or 1. dest names every index of 0 to 127 once.
All inputs are finite; a program needn't handle non-finite values.
Results may differ from the reference program's by a relative error of at most 0.0049.
Values may be sent and summed in bfloat16 or wider, within the bound.
No kernel may reach another device: no remote copies, remote signals or barrier semaphores. Data moves between devices by JAX's collectives and lax.ppermute only.
A program may use at most 128 MiB of HBM per device.

```python
import jax
import jax.numpy as jnp
from jax import lax

M = 768
NSEC = 8
PAIRS = 128


def touch_ends(array, stream_key, smallest, largest):
    shape = array.shape
    index_at = [jax.random.randint(jax.random.fold_in(stream_key, axis), (), 0, shape[axis]) for axis in range(len(shape))]
    array = array.at[tuple(index_at)].set(smallest)
    longest = shape.index(max(shape))
    index_at[longest] = (index_at[longest] + 1) % shape[longest]
    return array.at[tuple(index_at)].set(largest)


def steps_of(own_key, dims, split, smallest, high):
    def one(dim, parts):
        draws = jax.random.uniform(jax.random.fold_in(jax.random.fold_in(own_key, 6), dim), (parts,), jnp.float32, smallest / len(split), high / len(split))
        return jnp.repeat(jnp.exp(draws), dims[dim] // parts).reshape((-1,) + (1,) * (len(dims) - dim - 1))

    level = one(*split[0])
    for cut in split[1:]:
        level = level * one(*cut)
    return level


def noise(own_key, dims, scale, limit, shards=(), held_as=jnp.bfloat16):
    result = jax.random.normal(own_key, dims, jnp.float32) * scale
    if len(shards) > 0:
        result = steps_of(own_key, dims, shards, -0.22, 0.18) * result
    return jnp.clip(result, min=-limit, max=limit).astype(held_as)


def setup_inputs(seed: int = 0) -> dict:
    splits = jax.random.split(jax.random.key(seed), 6)
    return {
        "operators": noise(splits[0], (PAIRS, NSEC, M, M), 1.0, 6.0, ((0, 64), (1, 4))),
        "basis": noise(splits[1], (NSEC, M, M), M ** -0.5, 0.21875, ((0, 4),)),
        "shift": touch_ends(jax.random.randint(splits[2], (PAIRS,), -1, 2), jax.random.fold_in(splits[2], 1), -1, 1).astype(jnp.int32),
        "dest": jax.random.permutation(splits[3], PAIRS).astype(jnp.int32),
        "sector_sizes": touch_ends(jax.random.randint(splits[4], (NSEC,), M // 2, M + 1), jax.random.fold_in(splits[4], 1), M // 2, M).astype(jnp.int32),
    }


def reference(operators, basis, shift, dest, sector_sizes):
    columns = jnp.arange(M, dtype=jnp.int32)
    kept = columns[None, :] < sector_sizes[:, None]
    kept_basis = jnp.where(kept[:, None, :], basis, jnp.zeros_like(basis))
    sector_ids = jnp.arange(NSEC, dtype=jnp.int32)

    def rotate_pair(packed):
        blocks, offset = packed
        target = (sector_ids + offset) % NSEC

        def one_sector(index):
            block = lax.dynamic_index_in_dim(blocks, index, 0, False)
            own = lax.dynamic_index_in_dim(kept_basis, index, 0, False)
            other = lax.dynamic_index_in_dim(kept_basis, target[index], 0, False)
            half = jnp.dot(block, own, preferred_element_type=jnp.float32).astype(jnp.bfloat16)
            return jnp.dot(other.T, half, preferred_element_type=jnp.float32).astype(jnp.bfloat16)

        return lax.map(one_sector, sector_ids)

    rotated = lax.map(rotate_pair, (operators, shift))
    source = jnp.zeros((PAIRS,), jnp.int32).at[dest].set(jnp.arange(PAIRS, dtype=jnp.int32))
    return jnp.take(rotated, source, axis=0)
```

```python
import functools

import jax
import jax.numpy as jnp
from jax import lax
from jax.experimental import pallas as pl
from jax.experimental.pallas import tpu as pltpu
from jax.sharding import PartitionSpec as P

HBM = pl.BlockSpec(memory_space=pl.ANY)
VMEM = pl.BlockSpec(memory_space=pltpu.VMEM)
SMEM = pl.BlockSpec(memory_space=pltpu.SMEM)
LANES = 128
SUBLANES = 8
STEP = 16
TILE = 256


def times_transposed(left, right):
    return lax.dot_general(
        left, right, (((1,), (1,)), ((), ())), preferred_element_type=jnp.float32
    )


def layout_of(sizes_ref, sectors):
    heights = [pl.cdiv(sizes_ref[sector], STEP) * STEP for sector in range(sectors)]
    starts = [0]
    for height in heights:
        starts.append(starts[-1] + height)
    return heights, starts


def halve_kernel(
    sizes_ref, operators_ref, basis_ref, out_ref,
    blocks, own, turned, half, packed, block_sem, own_sem, out_sem,
):
    pairs, sectors, width = blocks.shape[0], blocks.shape[1], blocks.shape[3]
    count, rows = out_ref.shape[0], out_ref.shape[2]
    heights, starts = layout_of(sizes_ref, sectors)

    def fetch_own(sector):
        return pltpu.make_async_copy(
            basis_ref.at[sector], own.at[sector], own_sem.at[sector]
        )

    def fetch(pair, sector):
        return pltpu.make_async_copy(
            operators_ref.at[pair, sector],
            blocks.at[pair, sector],
            block_sem.at[pair * sectors + sector],
        )

    for pair in range(pairs):
        for sector in range(sectors):
            if pair == 0:
                fetch_own(sector).start()
            fetch(pair, sector).start()

    for pair in range(pairs):
        for sector in range(sectors):
            if pair == 0:
                fetch_own(sector).wait()
                for tile in range(width // TILE):
                    span = slice(tile * TILE, (tile + 1) * TILE)
                    index = tile * TILE + lax.broadcasted_iota(jnp.int32, (TILE, width), 0)
                    strip = own[sector, :, span].T
                    turned[sector, span, :] = jnp.where(
                        index < sizes_ref[sector], strip, jnp.zeros_like(strip)
                    )
            fetch(pair, sector).wait()

            @pl.loop(0, width // TILE)
            def _(tile):
                span = pl.ds(pl.multiple_of(tile * TILE, TILE), TILE)
                half[span, :] = times_transposed(
                    turned[sector, span, :], blocks[pair, sector]
                ).astype(half.dtype)

            @pl.loop(0, heights[sector] // STEP)
            def _(step):
                row = pl.multiple_of(step * STEP, STEP)
                for lane in range(width // LANES):
                    start = pl.multiple_of(
                        lane * starts[-1] + starts[sector] + row, STEP
                    )
                    packed[pair, pl.ds(start, STEP), :] = half[
                        pl.ds(row, STEP), lane * LANES : (lane + 1) * LANES
                    ]

        @pl.loop(0, count)
        def _(part):
            pltpu.make_async_copy(
                packed.at[pair, pl.ds(pl.multiple_of(part * rows, SUBLANES), rows)],
                out_ref.at[part, pair],
                out_sem,
            ).start()

    pltpu.make_async_copy(out_ref, out_ref, out_sem).wait()


def halve(sizes, operators, basis, count, rows):
    pairs, sectors, height, width = operators.shape
    dtype = operators.dtype
    return pl.pallas_call(
        halve_kernel,
        out_shape=jax.ShapeDtypeStruct((count, pairs, rows, LANES), dtype),
        in_specs=[SMEM, HBM, HBM],
        out_specs=HBM,
        scratch_shapes=[
            pltpu.VMEM(operators.shape, dtype),
            pltpu.VMEM(basis.shape, dtype),
            pltpu.VMEM((sectors, width, height), dtype),
            pltpu.VMEM((width, height), dtype),
            pltpu.VMEM((pairs, count * rows, LANES), dtype),
            pltpu.SemaphoreType.DMA((pairs * sectors,)),
            pltpu.SemaphoreType.DMA((sectors,)),
            pltpu.SemaphoreType.DMA,
        ],
        cost_estimate=pl.CostEstimate(
            flops=2 * operators.size * width,
            bytes_accessed=4 * operators.size,
            transcendentals=0,
        ),
        name="halve",
    )(sizes, operators, basis)


def reorder_kernel(dest_ref, in_ref, out_ref, out_sem):
    @pl.loop(0, in_ref.shape[0])
    def _(pair):
        pltpu.make_async_copy(
            in_ref.at[pair], out_ref.at[dest_ref[pair]], out_sem
        ).start()

    pltpu.make_async_copy(out_ref, out_ref, out_sem).wait()


def reorder(blocks, dest):
    return pl.pallas_call(
        reorder_kernel,
        out_shape=jax.ShapeDtypeStruct(blocks.shape, blocks.dtype),
        in_specs=[SMEM, VMEM],
        out_specs=HBM,
        scratch_shapes=[pltpu.SemaphoreType.DMA],
        cost_estimate=pl.CostEstimate(
            flops=0, bytes_accessed=4 * blocks.size, transcendentals=0
        ),
        name="reorder",
    )(dest, blocks)


def finish_kernel(
    sizes_ref, offset_ref, strips_ref, turned_ref, out_ref,
    packed, target, half, result, in_sem, target_sem, out_sem,
):
    pairs, sectors, width = result.shape[0], result.shape[1], result.shape[3]
    count, rows = strips_ref.shape[0], strips_ref.shape[2]
    heights, starts = layout_of(sizes_ref, sectors)

    def fetch(pair, sector):
        slot = pair * sectors + sector
        return pltpu.make_async_copy(
            turned_ref.at[sector + 1 + offset_ref[pair]],
            target.at[slot],
            target_sem.at[slot],
        )

    for pair in range(pairs):

        @pl.loop(0, count)
        def _(part):
            pltpu.make_async_copy(
                strips_ref.at[part, pair],
                packed.at[pair, pl.ds(pl.multiple_of(part * rows, SUBLANES), rows)],
                in_sem.at[pair],
            ).start()

        for sector in range(sectors):
            fetch(pair, sector).start()

    for pair in range(pairs):
        pltpu.make_async_copy(packed.at[pair], packed.at[pair], in_sem.at[pair]).wait()
        for sector in range(sectors):

            @pl.loop(0, heights[sector] // STEP)
            def _(step):
                row = pl.multiple_of(step * STEP, STEP)
                for lane in range(width // LANES):
                    start = pl.multiple_of(
                        lane * starts[-1] + starts[sector] + row, STEP
                    )
                    half[pl.ds(row, STEP), lane * LANES : (lane + 1) * LANES] = packed[
                        pair, pl.ds(start, STEP), :
                    ]

            @pl.loop(heights[sector] // STEP, width // STEP)
            def _(step):
                row = pl.multiple_of(step * STEP, STEP)
                half[pl.ds(row, STEP), :] = jnp.zeros((STEP, width), half.dtype)

            fetch(pair, sector).wait()

            @pl.loop(0, width // TILE)
            def _(tile):
                span = pl.ds(pl.multiple_of(tile * TILE, TILE), TILE)
                result[pair, sector, span, :] = times_transposed(
                    target[pair * sectors + sector, span, :], half[...]
                ).astype(result.dtype)
                pltpu.make_async_copy(
                    result.at[pair, sector, span], out_ref.at[pair, sector, span], out_sem
                ).start()

    pltpu.make_async_copy(out_ref, out_ref, out_sem).wait()


def finish(sizes, offsets, strips, turned, shape):
    pairs, sectors, height, width = shape
    count, _, rows, _ = strips.shape
    dtype = strips.dtype
    size = pairs * sectors * height * width
    return pl.pallas_call(
        finish_kernel,
        out_shape=jax.ShapeDtypeStruct(shape, dtype),
        in_specs=[SMEM, SMEM, VMEM, HBM],
        out_specs=HBM,
        scratch_shapes=[
            pltpu.VMEM((pairs, count * rows, LANES), dtype),
            pltpu.VMEM((pairs * sectors, height, width), dtype),
            pltpu.VMEM((width, height), dtype),
            pltpu.VMEM(shape, dtype),
            pltpu.SemaphoreType.DMA((pairs,)),
            pltpu.SemaphoreType.DMA((pairs * sectors,)),
            pltpu.SemaphoreType.DMA,
        ],
        cost_estimate=pl.CostEstimate(
            flops=2 * size * width, bytes_accessed=6 * size, transcendentals=0
        ),
        name="finish",
    )(sizes, offsets, strips, turned)


def body(operators, basis, shift, dest, sector_sizes):
    pairs, sectors, width = operators.shape[0], operators.shape[1], operators.shape[3]
    count = lax.axis_size("ops")
    sec_count = lax.axis_size("sec")
    total = sectors * sec_count
    sec_pos, ops_pos = lax.axis_index("sec"), lax.axis_index("ops")
    rows = sectors * width * width // (LANES * count)

    own_sizes = lax.dynamic_slice_in_dim(sector_sizes, sec_pos * sectors, sectors)
    strips = halve(own_sizes, operators, basis, count, rows)
    spread = lax.all_to_all(strips, "ops", 0, 0, tiled=True)

    forward = [(i, (i + 1) % sec_count) for i in range(sec_count)]
    backward = [(j, i) for i, j in forward]
    low = lax.ppermute(basis[-1:], "sec", forward)
    high = lax.ppermute(basis[:1], "sec", backward)
    near = jnp.concatenate([low, basis, high], axis=0)
    near_ids = (sec_pos * sectors - 1 + jnp.arange(sectors + 2, dtype=jnp.int32)) % total
    sizes = jnp.sum(
        jnp.where(
            near_ids[:, None] == jnp.arange(total, dtype=jnp.int32)[None, :],
            sector_sizes[None, :],
            0,
        ),
        axis=1,
    )
    kept = jnp.arange(width, dtype=jnp.int32)[None, :] < sizes[:, None]
    turned = jnp.swapaxes(jnp.where(kept[:, None, :], near, jnp.zeros_like(near)), 1, 2)
    mine = ops_pos * pairs + jnp.arange(pairs, dtype=jnp.int32)
    offsets = jnp.sum(jnp.where(mine[:, None] == dest[None, :], shift[None, :], 0), axis=1)

    ordered = reorder(spread.reshape((count * pairs,) + spread.shape[2:]), dest)
    back = lax.all_to_all(ordered.reshape(spread.shape), "ops", 0, 0, tiled=True)
    return finish(own_sizes, offsets, back, turned, operators.shape)


def solution(mesh):
    return jax.shard_map(
        body,
        mesh=mesh,
        in_specs=(P("ops", "sec", None, None), P("sec", None, None), P(), P(), P()),
        out_specs=P("ops", "sec", None, None),
        check_vma=False,
    )
```

```python
import functools

import jax
import jax.numpy as jnp
from jax import lax
from jax.experimental import pallas as pl
from jax.experimental.pallas import tpu as pltpu
from jax.sharding import PartitionSpec as P

HBM = pl.BlockSpec(memory_space=pl.ANY)
VMEM = pl.BlockSpec(memory_space=pltpu.VMEM)
SMEM = pl.BlockSpec(memory_space=pltpu.SMEM)
LANES = 128
SUBLANES = 8
STEP = 16
TILE = 256
CHOICES = 4


def times_transposed(left, right):
    return lax.dot_general(
        left, right, (((1,), (1,)), ((), ())), preferred_element_type=jnp.float32
    )


def regions_of(sizes_ref, sectors, lanes):
    first = lax.axis_index("sec") * sectors
    heights = [
        pl.cdiv(sizes_ref[first + sector], STEP) * STEP for sector in range(sectors)
    ]
    return first, lambda sector: (
        sum(
            jnp.where(other < sector, lanes * height, 0)
            for other, height in enumerate(heights)
        ),
        sum(
            jnp.where(other == sector, height, 0) for other, height in enumerate(heights)
        ),
    )


def halve_kernel(
    sizes_ref, operators_ref, basis_ref, out_ref,
    blocks, own, turned, packed, block_sem, own_sem, out_sem,
):
    pairs, sectors, width = blocks.shape[0], blocks.shape[1], blocks.shape[3]
    count, rows = out_ref.shape[0], out_ref.shape[2]
    first, region = regions_of(sizes_ref, sectors, width // LANES)

    def fetch_own(sector):
        return pltpu.make_async_copy(
            basis_ref.at[sector], own.at[sector], own_sem.at[sector]
        )

    def fetch(pair, sector):
        return pltpu.make_async_copy(
            operators_ref.at[pair, sector],
            blocks.at[pair, sector],
            block_sem.at[pair * sectors + sector],
        )

    for pair in range(pairs):
        for sector in range(sectors):
            if pair == 0:
                fetch_own(sector).start()
            fetch(pair, sector).start()

    @pl.loop(0, pairs * sectors)
    def _(index):
        pair, sector = index // sectors, index % sectors
        start, height = region(sector)

        @pl.when(pair == 0)
        def _():
            fetch_own(sector).wait()
            for tile in range(width // TILE):
                span = slice(tile * TILE, (tile + 1) * TILE)
                place = tile * TILE + lax.broadcasted_iota(jnp.int32, (TILE, width), 0)
                strip = own[sector, :, span].T
                turned[sector, span, :] = jnp.where(
                    place < sizes_ref[first + sector], strip, jnp.zeros_like(strip)
                )

        fetch(pair, sector).wait()
        for tile in range(width // TILE):
            half = times_transposed(
                turned[sector], blocks[pair, sector, tile * TILE : (tile + 1) * TILE, :]
            ).astype(packed.dtype)
            for side in range(TILE // LANES):
                lane = tile * (TILE // LANES) + side
                packed[pair, pl.ds(pl.multiple_of(start + lane * height, STEP), width), :] = (
                    half[:, side * LANES : (side + 1) * LANES]
                )

        @pl.when(sector == sectors - 1)
        def _():
            @pl.loop(0, count)
            def _(part):
                pltpu.make_async_copy(
                    packed.at[pair, pl.ds(pl.multiple_of(part * rows, SUBLANES), rows)],
                    out_ref.at[part, pair],
                    out_sem,
                ).start()

    pltpu.make_async_copy(out_ref, out_ref, out_sem).wait()


def halve(sizes, operators, basis, count, rows):
    pairs, sectors, height, width = operators.shape
    dtype = operators.dtype
    return pl.pallas_call(
        halve_kernel,
        out_shape=jax.ShapeDtypeStruct((count, pairs, rows, LANES), dtype),
        in_specs=[SMEM, HBM, HBM],
        out_specs=HBM,
        scratch_shapes=[
            pltpu.VMEM(operators.shape, dtype),
            pltpu.VMEM(basis.shape, dtype),
            pltpu.VMEM((sectors, width, height), dtype),
            pltpu.VMEM((pairs, count * rows + width, LANES), dtype),
            pltpu.SemaphoreType.DMA((pairs * sectors,)),
            pltpu.SemaphoreType.DMA((sectors,)),
            pltpu.SemaphoreType.DMA,
        ],
        cost_estimate=pl.CostEstimate(
            flops=2 * operators.size * width,
            bytes_accessed=4 * operators.size,
            transcendentals=0,
        ),
        name="halve",
    )(sizes, operators, basis)


def finish_kernel(
    sizes_ref, offset_ref, strips_ref, turned_ref, out_ref,
    packed, target, half, result, in_sem, target_sem, out_sem,
):
    pairs, sectors, width = result.shape[0], result.shape[1], result.shape[3]
    count, rows = strips_ref.shape[0], strips_ref.shape[2]
    _, region = regions_of(sizes_ref, sectors, width // LANES)

    def fetch(pair, sector):
        slot = pair * sectors + sector
        return pltpu.make_async_copy(
            turned_ref.at[sector + 1 + offset_ref[pair]],
            target.at[slot],
            target_sem.at[slot],
        )

    for pair in range(pairs):

        @pl.loop(0, count)
        def _(part):
            pltpu.make_async_copy(
                strips_ref.at[part, pair],
                packed.at[pair, pl.ds(pl.multiple_of(part * rows, SUBLANES), rows)],
                in_sem.at[pair],
            ).start()

        for sector in range(sectors):
            fetch(pair, sector).start()

    @pl.loop(0, pairs * sectors)
    def _(index):
        pair, sector = index // sectors, index % sectors
        start, height = region(sector)

        @pl.when(sector == 0)
        def _():
            whole = packed.at[pair, pl.ds(0, count * rows)]
            pltpu.make_async_copy(whole, whole, in_sem.at[pair]).wait()

        for lane in range(width // LANES):
            half[:, lane * LANES : (lane + 1) * LANES] = packed[
                pair, pl.ds(pl.multiple_of(start + lane * height, STEP), width), :
            ]

        @pl.loop(height // STEP, width // STEP)
        def _(step):
            row = pl.multiple_of(step * STEP, STEP)
            half[pl.ds(row, STEP), :] = jnp.zeros((STEP, width), half.dtype)

        fetch(pair, sector).wait()
        for tile in range(width // TILE):
            span = slice(tile * TILE, (tile + 1) * TILE)
            result[pair, sector, :, span] = times_transposed(
                target[index], half[span, :]
            ).astype(result.dtype)
        pltpu.make_async_copy(
            result.at[pair, sector], out_ref.at[pair, sector], out_sem
        ).start()

    pltpu.make_async_copy(out_ref, out_ref, out_sem).wait()


def finish(sizes, offsets, strips, turned, shape):
    pairs, sectors, height, width = shape
    count, _, rows, _ = strips.shape
    dtype = strips.dtype
    size = pairs * sectors * height * width
    return pl.pallas_call(
        finish_kernel,
        out_shape=jax.ShapeDtypeStruct(shape, dtype),
        in_specs=[SMEM, SMEM, HBM, HBM],
        out_specs=HBM,
        scratch_shapes=[
            pltpu.VMEM((pairs, count * rows + width, LANES), dtype),
            pltpu.VMEM((pairs * sectors, height, width), dtype),
            pltpu.VMEM((width, height), dtype),
            pltpu.VMEM(shape, dtype),
            pltpu.SemaphoreType.DMA((pairs,)),
            pltpu.SemaphoreType.DMA((pairs * sectors,)),
            pltpu.SemaphoreType.DMA,
        ],
        cost_estimate=pl.CostEstimate(
            flops=2 * size * width, bytes_accessed=6 * size, transcendentals=0
        ),
        name="finish",
    )(sizes, offsets, strips, turned)


def reorder_kernel(dest_ref, in_ref, out_ref, held, in_sem, out_sem):
    parts = in_sem.shape[0]
    per = in_ref.shape[0] // parts

    def fetch(part):
        span = pl.ds(part * per, per)
        return pltpu.make_async_copy(in_ref.at[span], held.at[span], in_sem.at[part])

    for part in range(parts):
        fetch(part).start()
    for part in range(parts):
        fetch(part).wait()

        @pl.loop(part * per, (part + 1) * per)
        def _(pair):
            pltpu.make_async_copy(
                held.at[pair], out_ref.at[dest_ref[pair]], out_sem
            ).start()

    pltpu.make_async_copy(out_ref, out_ref, out_sem).wait()


def reorder(blocks, dest):
    return pl.pallas_call(
        reorder_kernel,
        out_shape=jax.ShapeDtypeStruct(blocks.shape, blocks.dtype),
        in_specs=[SMEM, HBM],
        out_specs=HBM,
        scratch_shapes=[
            pltpu.VMEM(blocks.shape, blocks.dtype),
            pltpu.SemaphoreType.DMA((8,)),
            pltpu.SemaphoreType.DMA,
        ],
        cost_estimate=pl.CostEstimate(
            flops=0, bytes_accessed=4 * blocks.size, transcendentals=0
        ),
        name="reorder",
    )(dest, blocks)


def turned_basis(basis, sector_sizes):
    sectors, width = basis.shape[0], basis.shape[2]
    sec_count, sec_pos = lax.axis_size("sec"), lax.axis_index("sec")
    total = sectors * sec_count
    forward = [(i, (i + 1) % sec_count) for i in range(sec_count)]
    backward = [(j, i) for i, j in forward]
    low = lax.ppermute(basis[-1:], "sec", forward)
    high = lax.ppermute(basis[:1], "sec", backward)
    near = jnp.concatenate([low, basis, high], axis=0)
    near_ids = (sec_pos * sectors - 1 + jnp.arange(sectors + 2, dtype=jnp.int32)) % total
    sizes = jnp.sum(
        jnp.where(
            near_ids[:, None] == jnp.arange(total, dtype=jnp.int32)[None, :],
            sector_sizes[None, :],
            0,
        ),
        axis=1,
    )
    kept = jnp.arange(width, dtype=jnp.int32)[None, :] < sizes[:, None]
    return jnp.swapaxes(jnp.where(kept[:, None, :], near, jnp.zeros_like(near)), 1, 2)


def pipeline(rows, operators, basis, shift, dest, sector_sizes):
    pairs = operators.shape[0]
    count = lax.axis_size("ops")
    strips = halve(sector_sizes, operators, basis, count, rows)
    spread = lax.all_to_all(strips, "ops", 0, 0, tiled=True)
    turned = turned_basis(basis, sector_sizes)
    mine = lax.axis_index("ops") * pairs + jnp.arange(pairs, dtype=jnp.int32)
    offsets = jnp.sum(jnp.where(mine[:, None] == dest[None, :], shift[None, :], 0), axis=1)
    ordered = reorder(spread.reshape((count * pairs,) + spread.shape[2:]), dest)
    back = lax.all_to_all(ordered.reshape(spread.shape), "ops", 0, 0, tiled=True)
    return finish(sector_sizes, offsets, back, turned, operators.shape)


def body(operators, basis, shift, dest, sector_sizes):
    sectors, width = operators.shape[1], operators.shape[3]
    lanes, part = width // LANES, lax.axis_size("ops") * SUBLANES
    most = lanes * sectors * width // part
    least = most - CHOICES + 1
    heights = (sector_sizes + STEP - 1) // STEP * STEP
    longest = jnp.max(jnp.sum(heights.reshape(-1, sectors), axis=1)) * lanes
    choice = jnp.clip((longest + part - 1) // part - least, 0, CHOICES - 1)
    return lax.switch(
        choice,
        [
            functools.partial(pipeline, SUBLANES * tiles)
            for tiles in range(least, most + 1)
        ],
        operators, basis, shift, dest, sector_sizes,
    )


def solution(mesh):
    return jax.shard_map(
        body,
        mesh=mesh,
        in_specs=(P("ops", "sec", None, None), P("sec", None, None), P(), P(), P()),
        out_specs=P("ops", "sec", None, None),
        check_vma=False,
    )
```

```python
import functools

import jax
import jax.numpy as jnp
import numpy as np
from jax import lax
from jax.experimental import pallas as pl
from jax.experimental.pallas import tpu as pltpu
from jax.sharding import PartitionSpec as P

HBM = pl.BlockSpec(memory_space=pl.ANY)
VMEM = pl.BlockSpec(memory_space=pltpu.VMEM)
SMEM = pl.BlockSpec(memory_space=pltpu.SMEM)
LANES = 128
SUBLANES = 8
STEP = 16
TILE = 256
CHOICES = 4


def times_transposed(left, right):
    return lax.dot_general(
        left, right, (((1,), (1,)), ((), ())), preferred_element_type=jnp.float32
    )


def regions_of(sizes_ref, sectors, lanes):
    first = lax.axis_index("sec") * sectors
    heights = [
        pl.cdiv(sizes_ref[first + sector], STEP) * STEP for sector in range(sectors)
    ]
    return first, lambda sector: (
        sum(
            jnp.where(other < sector, lanes * height, 0)
            for other, height in enumerate(heights)
        ),
        sum(
            jnp.where(other == sector, height, 0) for other, height in enumerate(heights)
        ),
    )


def halve_kernel(
    sizes_ref, operators_ref, basis_ref, out_ref,
    blocks, own, turned, packed, block_sem, own_sem, out_sem,
):
    pairs, sectors, width = blocks.shape[0], blocks.shape[1], blocks.shape[3]
    count, rows = out_ref.shape[0], out_ref.shape[2]
    first, region = regions_of(sizes_ref, sectors, width // LANES)

    def fetch_own(sector):
        return pltpu.make_async_copy(
            basis_ref.at[sector], own.at[sector], own_sem.at[sector]
        )

    def fetch(pair, sector):
        return pltpu.make_async_copy(
            operators_ref.at[pair, sector],
            blocks.at[pair, sector],
            block_sem.at[pair * sectors + sector],
        )

    for pair in range(pairs):
        for sector in range(sectors):
            if pair == 0:
                fetch_own(sector).start()
            fetch(pair, sector).start()

    @pl.loop(0, pairs * sectors)
    def _(index):
        pair, sector = index // sectors, index % sectors
        start, height = region(sector)

        @pl.when(pair == 0)
        def _():
            fetch_own(sector).wait()
            for tile in range(width // TILE):
                span = slice(tile * TILE, (tile + 1) * TILE)
                place = tile * TILE + lax.broadcasted_iota(jnp.int32, (TILE, width), 0)
                strip = own[sector, :, span].T
                turned[sector, span, :] = jnp.where(
                    place < sizes_ref[first + sector], strip, jnp.zeros_like(strip)
                )

        fetch(pair, sector).wait()
        for tile in range(width // TILE):
            half = times_transposed(
                turned[sector], blocks[pair, sector, tile * TILE : (tile + 1) * TILE, :]
            ).astype(packed.dtype)
            for side in range(TILE // LANES):
                lane = tile * (TILE // LANES) + side
                packed[pair, pl.ds(pl.multiple_of(start + lane * height, STEP), width), :] = (
                    half[:, side * LANES : (side + 1) * LANES]
                )

        @pl.when(sector == sectors - 1)
        def _():
            @pl.loop(0, count)
            def _(part):
                pltpu.make_async_copy(
                    packed.at[pair, pl.ds(pl.multiple_of(part * rows, SUBLANES), rows)],
                    out_ref.at[part, pair],
                    out_sem,
                ).start()

    pltpu.make_async_copy(out_ref, out_ref, out_sem).wait()


def halve(sizes, operators, basis, count, rows):
    pairs, sectors, height, width = operators.shape
    dtype = operators.dtype
    return pl.pallas_call(
        halve_kernel,
        out_shape=jax.ShapeDtypeStruct((count, pairs, rows, LANES), dtype),
        in_specs=[SMEM, HBM, HBM],
        out_specs=HBM,
        scratch_shapes=[
            pltpu.VMEM(operators.shape, dtype),
            pltpu.VMEM(basis.shape, dtype),
            pltpu.VMEM((sectors, width, height), dtype),
            pltpu.VMEM((pairs, count * rows + width, LANES), dtype),
            pltpu.SemaphoreType.DMA((pairs * sectors,)),
            pltpu.SemaphoreType.DMA((sectors,)),
            pltpu.SemaphoreType.DMA,
        ],
        cost_estimate=pl.CostEstimate(
            flops=2 * operators.size * width,
            bytes_accessed=4 * operators.size,
            transcendentals=0,
        ),
        name="halve",
    )(sizes, operators, basis)


def finish_kernel(
    sizes_ref, offset_ref, strips_ref, turned_ref, out_ref,
    packed, target, half, result, in_sem, target_sem, out_sem,
):
    pairs, sectors, width = result.shape[0], result.shape[1], result.shape[3]
    count, rows = strips_ref.shape[0], strips_ref.shape[2]
    _, region = regions_of(sizes_ref, sectors, width // LANES)

    def fetch(pair, sector):
        slot = pair * sectors + sector
        return pltpu.make_async_copy(
            turned_ref.at[sector + 1 + offset_ref[pair]],
            target.at[slot],
            target_sem.at[slot],
        )

    for pair in range(pairs):

        @pl.loop(0, count)
        def _(part):
            pltpu.make_async_copy(
                strips_ref.at[part, pair],
                packed.at[pair, pl.ds(pl.multiple_of(part * rows, SUBLANES), rows)],
                in_sem.at[pair],
            ).start()

        for sector in range(sectors):
            fetch(pair, sector).start()

    @pl.loop(0, pairs * sectors)
    def _(index):
        pair, sector = index // sectors, index % sectors
        start, height = region(sector)

        @pl.when(sector == 0)
        def _():
            whole = packed.at[pair, pl.ds(0, count * rows)]
            pltpu.make_async_copy(whole, whole, in_sem.at[pair]).wait()

        for lane in range(width // LANES):
            half[:, lane * LANES : (lane + 1) * LANES] = packed[
                pair, pl.ds(pl.multiple_of(start + lane * height, STEP), width), :
            ]

        @pl.loop(height // STEP, width // STEP)
        def _(step):
            row = pl.multiple_of(step * STEP, STEP)
            half[pl.ds(row, STEP), :] = jnp.zeros((STEP, width), half.dtype)

        fetch(pair, sector).wait()
        for tile in range(width // TILE):
            span = slice(tile * TILE, (tile + 1) * TILE)
            result[pair, sector, :, span] = times_transposed(
                target[index], half[span, :]
            ).astype(result.dtype)
            pltpu.make_async_copy(
                result.at[pair, sector, :, span], out_ref.at[pair, sector, :, span], out_sem
            ).start()

    pltpu.make_async_copy(out_ref, out_ref, out_sem).wait()


def finish(sizes, offsets, strips, turned, shape):
    pairs, sectors, height, width = shape
    count, _, rows, _ = strips.shape
    dtype = strips.dtype
    size = pairs * sectors * height * width
    return pl.pallas_call(
        finish_kernel,
        out_shape=jax.ShapeDtypeStruct(shape, dtype),
        in_specs=[SMEM, SMEM, HBM, HBM],
        out_specs=HBM,
        scratch_shapes=[
            pltpu.VMEM((pairs, count * rows + width, LANES), dtype),
            pltpu.VMEM((pairs * sectors, height, width), dtype),
            pltpu.VMEM((width, height), dtype),
            pltpu.VMEM(shape, dtype),
            pltpu.SemaphoreType.DMA((pairs,)),
            pltpu.SemaphoreType.DMA((pairs * sectors,)),
            pltpu.SemaphoreType.DMA,
        ],
        cost_estimate=pl.CostEstimate(
            flops=2 * size * width, bytes_accessed=6 * size, transcendentals=0
        ),
        name="finish",
    )(sizes, offsets, strips, turned)


def reorder_kernel(dest_ref, in_ref, out_ref, out_sem):
    @pl.loop(0, in_ref.shape[0])
    def _(pair):
        pltpu.make_async_copy(
            in_ref.at[pair], out_ref.at[dest_ref[pair]], out_sem
        ).start()

    pltpu.make_async_copy(out_ref, out_ref, out_sem).wait()


def reorder(blocks, dest):
    return pl.pallas_call(
        reorder_kernel,
        out_shape=jax.ShapeDtypeStruct(blocks.shape, blocks.dtype),
        in_specs=[SMEM, HBM],
        out_specs=HBM,
        scratch_shapes=[pltpu.SemaphoreType.DMA],
        cost_estimate=pl.CostEstimate(
            flops=0, bytes_accessed=4 * blocks.size, transcendentals=0
        ),
        compiler_params=pltpu.CompilerParams(vmem_limit_bytes=8 << 20),
        name="reorder",
    )(dest, blocks)


def turned_basis(basis, sector_sizes):
    sectors, width = basis.shape[0], basis.shape[2]
    sec_count, sec_pos = lax.axis_size("sec"), lax.axis_index("sec")
    total = sectors * sec_count
    forward = [(i, (i + 1) % sec_count) for i in range(sec_count)]
    backward = [(j, i) for i, j in forward]
    low = lax.ppermute(basis[-1:], "sec", forward)
    high = lax.ppermute(basis[:1], "sec", backward)
    near = jnp.concatenate([low, basis, high], axis=0)
    near_ids = (sec_pos * sectors - 1 + jnp.arange(sectors + 2, dtype=jnp.int32)) % total
    sizes = jnp.sum(
        jnp.where(
            near_ids[:, None] == jnp.arange(total, dtype=jnp.int32)[None, :],
            sector_sizes[None, :],
            0,
        ),
        axis=1,
    )
    kept = jnp.arange(width, dtype=jnp.int32)[None, :] < sizes[:, None]
    return jnp.swapaxes(jnp.where(kept[:, None, :], near, jnp.zeros_like(near)), 1, 2)


def pipeline(rows, operators, basis, shift, dest, sector_sizes):
    pairs = operators.shape[0]
    count = lax.axis_size("ops")
    strips = halve(sector_sizes, operators, basis, count, rows)
    spread = lax.all_to_all(strips, "ops", 0, 0, tiled=True)
    turned = turned_basis(basis, sector_sizes)
    mine = lax.axis_index("ops") * pairs + jnp.arange(pairs, dtype=jnp.int32)
    offsets = jnp.sum(jnp.where(mine[:, None] == dest[None, :], shift[None, :], 0), axis=1)
    spread, turned, offsets = lax.optimization_barrier((spread, turned, offsets))
    ordered = reorder(spread.reshape((count * pairs,) + spread.shape[2:]), dest)
    back = lax.all_to_all(ordered.reshape(spread.shape), "ops", 0, 0, tiled=True)
    return finish(sector_sizes, offsets, back, turned, operators.shape)


def body(operators, basis, shift, dest, sector_sizes):
    sectors, width = operators.shape[1], operators.shape[3]
    lanes, part = width // LANES, lax.axis_size("ops") * SUBLANES
    most = lanes * sectors * width // part
    least = most - CHOICES + 1
    heights = (sector_sizes + STEP - 1) // STEP * STEP
    places = np.arange(heights.shape[0])
    groups = places // sectors
    mates = (groups[:, None] == groups[None, :]) & (places[:, None] < places[None, :])
    assert sectors == 2
    longest = lanes * jnp.max(jnp.where(mates, heights[:, None] + heights[None, :], 0))
    choice = jnp.clip((longest + part - 1) // part - least, 0, CHOICES - 1)
    return lax.switch(
        choice,
        [
            functools.partial(pipeline, SUBLANES * tiles)
            for tiles in range(least, most + 1)
        ],
        operators, basis, shift, dest, sector_sizes,
    )


def solution(mesh):
    return jax.shard_map(
        body,
        mesh=mesh,
        in_specs=(P("ops", "sec", None, None), P("sec", None, None), P(), P(), P()),
        out_specs=P("ops", "sec", None, None),
        check_vma=False,
    )
```

```python
import functools

import jax
import jax.numpy as jnp
from jax import lax
from jax.experimental import pallas as pl
from jax.experimental.pallas import tpu as pltpu
from jax.sharding import PartitionSpec as P

HBM = pl.BlockSpec(memory_space=pl.ANY)
VMEM = pl.BlockSpec(memory_space=pltpu.VMEM)
SMEM = pl.BlockSpec(memory_space=pltpu.SMEM)
LANES = 128
SUBLANES = 8
STEP = 16
TILE = 256
CHOICES = 4


def times_transposed(left, right):
    return lax.dot_general(
        left, right, (((1,), (1,)), ((), ())), preferred_element_type=jnp.float32
    )


def regions_of(sizes_ref, sectors, lanes):
    first = lax.axis_index("sec") * sectors
    heights = [
        pl.cdiv(sizes_ref[first + sector], STEP) * STEP for sector in range(sectors)
    ]
    return first, lambda sector: (
        sum(
            jnp.where(other < sector, lanes * height, 0)
            for other, height in enumerate(heights)
        ),
        sum(
            jnp.where(other == sector, height, 0) for other, height in enumerate(heights)
        ),
    )


def halve_kernel(
    sizes_ref, operators_ref, basis_ref, out_ref,
    blocks, own, turned, packed, block_sem, own_sem, out_sem,
):
    pairs, sectors, width = blocks.shape[0], blocks.shape[1], blocks.shape[3]
    count, rows = out_ref.shape[0], out_ref.shape[2]
    first, region = regions_of(sizes_ref, sectors, width // LANES)

    def fetch_own(sector):
        return pltpu.make_async_copy(
            basis_ref.at[sector], own.at[sector], own_sem.at[sector]
        )

    def fetch(pair, sector):
        return pltpu.make_async_copy(
            operators_ref.at[pair, sector],
            blocks.at[pair, sector],
            block_sem.at[pair * sectors + sector],
        )

    for pair in range(pairs):
        for sector in range(sectors):
            if pair == 0:
                fetch_own(sector).start()
            fetch(pair, sector).start()

    @pl.loop(0, pairs * sectors)
    def _(index):
        pair, sector = index // sectors, index % sectors
        start, height = region(sector)

        @pl.when(pair == 0)
        def _():
            fetch_own(sector).wait()
            for tile in range(width // TILE):
                span = slice(tile * TILE, (tile + 1) * TILE)
                place = tile * TILE + lax.broadcasted_iota(jnp.int32, (TILE, width), 0)
                strip = own[sector, :, span].T
                turned[sector, span, :] = jnp.where(
                    place < sizes_ref[first + sector], strip, jnp.zeros_like(strip)
                )

        fetch(pair, sector).wait()
        for tile in range(width // TILE):
            half = times_transposed(
                turned[sector], blocks[pair, sector, tile * TILE : (tile + 1) * TILE, :]
            ).astype(packed.dtype)
            for side in range(TILE // LANES):
                lane = tile * (TILE // LANES) + side
                packed[pair, pl.ds(pl.multiple_of(start + lane * height, STEP), width), :] = (
                    half[:, side * LANES : (side + 1) * LANES]
                )

        @pl.when(sector == sectors - 1)
        def _():
            @pl.loop(0, count)
            def _(part):
                pltpu.make_async_copy(
                    packed.at[pair, pl.ds(pl.multiple_of(part * rows, SUBLANES), rows)],
                    out_ref.at[part, pair],
                    out_sem,
                ).start()

    pltpu.make_async_copy(out_ref, out_ref, out_sem).wait()


def halve(sizes, operators, basis, count, rows):
    pairs, sectors, height, width = operators.shape
    dtype = operators.dtype
    return pl.pallas_call(
        halve_kernel,
        out_shape=jax.ShapeDtypeStruct((count, pairs, rows, LANES), dtype),
        in_specs=[SMEM, HBM, HBM],
        out_specs=HBM,
        scratch_shapes=[
            pltpu.VMEM(operators.shape, dtype),
            pltpu.VMEM(basis.shape, dtype),
            pltpu.VMEM((sectors, width, height), dtype),
            pltpu.VMEM((pairs, count * rows + width, LANES), dtype),
            pltpu.SemaphoreType.DMA((pairs * sectors,)),
            pltpu.SemaphoreType.DMA((sectors,)),
            pltpu.SemaphoreType.DMA,
        ],
        cost_estimate=pl.CostEstimate(
            flops=2 * operators.size * width,
            bytes_accessed=4 * operators.size,
            transcendentals=0,
        ),
        name="halve",
    )(sizes, operators, basis)


def finish_kernel(
    sizes_ref, offset_ref, strips_ref, turned_ref, out_ref,
    packed, target, half, result, in_sem, target_sem, out_sem,
):
    pairs, sectors, width = result.shape[0], result.shape[1], result.shape[3]
    count, rows = strips_ref.shape[0], strips_ref.shape[2]
    _, region = regions_of(sizes_ref, sectors, width // LANES)

    def fetch(pair, sector):
        slot = pair * sectors + sector
        return pltpu.make_async_copy(
            turned_ref.at[sector + 1 + offset_ref[pair]],
            target.at[slot],
            target_sem.at[slot],
        )

    for pair in range(pairs):

        @pl.loop(0, count)
        def _(part):
            pltpu.make_async_copy(
                strips_ref.at[part, pair],
                packed.at[pair, pl.ds(pl.multiple_of(part * rows, SUBLANES), rows)],
                in_sem.at[pair],
            ).start()

        for sector in range(sectors):
            fetch(pair, sector).start()

    @pl.loop(0, pairs * sectors)
    def _(index):
        pair, sector = index // sectors, index % sectors
        start, height = region(sector)

        @pl.when(sector == 0)
        def _():
            whole = packed.at[pair, pl.ds(0, count * rows)]
            pltpu.make_async_copy(whole, whole, in_sem.at[pair]).wait()

        for lane in range(width // LANES):
            half[:, lane * LANES : (lane + 1) * LANES] = packed[
                pair, pl.ds(pl.multiple_of(start + lane * height, STEP), width), :
            ]

        @pl.loop(height // STEP, width // STEP)
        def _(step):
            row = pl.multiple_of(step * STEP, STEP)
            half[pl.ds(row, STEP), :] = jnp.zeros((STEP, width), half.dtype)

        fetch(pair, sector).wait()
        for tile in range(width // TILE):
            span = slice(tile * TILE, (tile + 1) * TILE)
            result[pair, sector, :, span] = times_transposed(
                target[index], half[span, :]
            ).astype(result.dtype)
            pltpu.make_async_copy(
                result.at[pair, sector, :, span], out_ref.at[pair, sector, :, span], out_sem
            ).start()

    pltpu.make_async_copy(out_ref, out_ref, out_sem).wait()


def finish(sizes, offsets, strips, turned, shape):
    pairs, sectors, height, width = shape
    count, _, rows, _ = strips.shape
    dtype = strips.dtype
    size = pairs * sectors * height * width
    return pl.pallas_call(
        finish_kernel,
        out_shape=jax.ShapeDtypeStruct(shape, dtype),
        in_specs=[SMEM, SMEM, HBM, HBM],
        out_specs=HBM,
        scratch_shapes=[
            pltpu.VMEM((pairs, count * rows + width, LANES), dtype),
            pltpu.VMEM((pairs * sectors, height, width), dtype),
            pltpu.VMEM((width, height), dtype),
            pltpu.VMEM(shape, dtype),
            pltpu.SemaphoreType.DMA((pairs,)),
            pltpu.SemaphoreType.DMA((pairs * sectors,)),
            pltpu.SemaphoreType.DMA,
        ],
        cost_estimate=pl.CostEstimate(
            flops=2 * size * width, bytes_accessed=6 * size, transcendentals=0
        ),
        compiler_params=pltpu.CompilerParams(vmem_limit_bytes=24 << 20),
        name="finish",
    )(sizes, offsets, strips, turned)


def reorder_kernel(dest_ref, in_ref, out_ref, out_sem):
    @pl.loop(0, in_ref.shape[0])
    def _(pair):
        pltpu.make_async_copy(
            in_ref.at[pair], out_ref.at[dest_ref[pair]], out_sem
        ).start()

    pltpu.make_async_copy(out_ref, out_ref, out_sem).wait()


def reorder(blocks, dest):
    return pl.pallas_call(
        reorder_kernel,
        out_shape=jax.ShapeDtypeStruct(blocks.shape, blocks.dtype),
        in_specs=[SMEM, HBM],
        out_specs=HBM,
        scratch_shapes=[pltpu.SemaphoreType.DMA],
        cost_estimate=pl.CostEstimate(
            flops=0, bytes_accessed=4 * blocks.size, transcendentals=0
        ),
        compiler_params=pltpu.CompilerParams(vmem_limit_bytes=8 << 20),
        name="reorder",
    )(dest, blocks)


def turned_basis(basis, sector_sizes):
    sectors, width = basis.shape[0], basis.shape[2]
    sec_count, sec_pos = lax.axis_size("sec"), lax.axis_index("sec")
    total = sectors * sec_count
    forward = [(i, (i + 1) % sec_count) for i in range(sec_count)]
    backward = [(j, i) for i, j in forward]
    low = lax.ppermute(basis[-1:], "sec", forward)
    high = lax.ppermute(basis[:1], "sec", backward)
    near = jnp.concatenate([low, basis, high], axis=0)
    near_ids = (sec_pos * sectors - 1 + jnp.arange(sectors + 2, dtype=jnp.int32)) % total
    sizes = jnp.sum(
        jnp.where(
            near_ids[:, None] == jnp.arange(total, dtype=jnp.int32)[None, :],
            sector_sizes[None, :],
            0,
        ),
        axis=1,
    )
    kept = jnp.arange(width, dtype=jnp.int32)[None, :] < sizes[:, None]
    return jnp.swapaxes(jnp.where(kept[:, None, :], near, jnp.zeros_like(near)), 1, 2)


def pipeline(rows, operators, basis, shift, dest, sector_sizes):
    pairs = operators.shape[0]
    count = lax.axis_size("ops")
    strips = halve(sector_sizes, operators, basis, count, rows)
    spread = lax.all_to_all(strips, "ops", 0, 0, tiled=True)
    turned = turned_basis(basis, sector_sizes)
    mine = lax.axis_index("ops") * pairs + jnp.arange(pairs, dtype=jnp.int32)
    offsets = jnp.sum(jnp.where(mine[:, None] == dest[None, :], shift[None, :], 0), axis=1)
    spread, turned, offsets = lax.optimization_barrier((spread, turned, offsets))
    ordered = reorder(spread.reshape((count * pairs,) + spread.shape[2:]), dest)
    back = lax.all_to_all(ordered.reshape(spread.shape), "ops", 0, 0, tiled=True)
    return finish(sector_sizes, offsets, back, turned, operators.shape)


def body(operators, basis, shift, dest, sector_sizes):
    sectors, width = operators.shape[1], operators.shape[3]
    lanes, part = width // LANES, lax.axis_size("ops") * SUBLANES
    most = lanes * sectors * width // part
    least = most - CHOICES + 1
    heights = (sector_sizes + STEP - 1) // STEP * STEP
    longest = jnp.max(jnp.sum(heights.reshape(-1, sectors), axis=1)) * lanes
    choice = jnp.clip((longest + part - 1) // part - least, 0, CHOICES - 1)
    return lax.switch(
        choice,
        [
            functools.partial(pipeline, SUBLANES * tiles)
            for tiles in range(least, most + 1)
        ],
        operators, basis, shift, dest, sector_sizes,
    )


def solution(mesh):
    return jax.shard_map(
        body,
        mesh=mesh,
        in_specs=(P("ops", "sec", None, None), P("sec", None, None), P(), P(), P()),
        out_specs=P("ops", "sec", None, None),
        check_vma=False,
    )
```

```python
import functools

import jax
import jax.numpy as jnp
from jax import lax
from jax.experimental import pallas as pl
from jax.experimental.pallas import tpu as pltpu
from jax.sharding import PartitionSpec as P

HBM = pl.BlockSpec(memory_space=pl.ANY)
VMEM = pl.BlockSpec(memory_space=pltpu.VMEM)
SMEM = pl.BlockSpec(memory_space=pltpu.SMEM)
LANES = 128
SUBLANES = 8
STEP = 16
TILE = 256
CHOICES = 4


def times_transposed(left, right):
    return lax.dot_general(
        left, right, (((1,), (1,)), ((), ())), preferred_element_type=jnp.float32
    )


def regions_of(sizes_ref, sectors, lanes):
    first = lax.axis_index("sec") * sectors
    heights = [
        pl.cdiv(sizes_ref[first + sector], STEP) * STEP for sector in range(sectors)
    ]
    return first, lambda sector: (
        sum(
            jnp.where(other < sector, lanes * height, 0)
            for other, height in enumerate(heights)
        ),
        sum(
            jnp.where(other == sector, height, 0) for other, height in enumerate(heights)
        ),
    )


def halve_kernel(
    sizes_hbm, operators_ref, basis_ref, out_ref,
    sizes_ref, blocks, own, turned, packed, size_sem, block_sem, own_sem, out_sem,
):
    pairs, sectors, width = blocks.shape[0], blocks.shape[1], blocks.shape[3]
    count, rows = out_ref.shape[0], out_ref.shape[2]
    sizes_copy = pltpu.make_async_copy(sizes_hbm, sizes_ref, size_sem)
    sizes_copy.start()

    def fetch_own(sector):
        return pltpu.make_async_copy(
            basis_ref.at[sector], own.at[sector], own_sem.at[sector]
        )

    def fetch(pair, sector):
        return pltpu.make_async_copy(
            operators_ref.at[pair, sector],
            blocks.at[pair, sector],
            block_sem.at[pair * sectors + sector],
        )

    for pair in range(pairs):
        for sector in range(sectors):
            if pair == 0:
                fetch_own(sector).start()
            fetch(pair, sector).start()

    sizes_copy.wait()
    first, region = regions_of(sizes_ref, sectors, width // LANES)

    @pl.loop(0, pairs * sectors)
    def _(index):
        pair, sector = index // sectors, index % sectors
        start, height = region(sector)

        @pl.when(pair == 0)
        def _():
            fetch_own(sector).wait()
            for tile in range(width // TILE):
                span = slice(tile * TILE, (tile + 1) * TILE)
                place = tile * TILE + lax.broadcasted_iota(jnp.int32, (TILE, width), 0)
                strip = own[sector, :, span].T
                turned[sector, span, :] = jnp.where(
                    place < sizes_ref[first + sector], strip, jnp.zeros_like(strip)
                )

        fetch(pair, sector).wait()
        for tile in range(width // TILE):
            half = times_transposed(
                turned[sector], blocks[pair, sector, tile * TILE : (tile + 1) * TILE, :]
            ).astype(packed.dtype)
            for side in range(TILE // LANES):
                lane = tile * (TILE // LANES) + side
                packed[pair, pl.ds(pl.multiple_of(start + lane * height, STEP), width), :] = (
                    half[:, side * LANES : (side + 1) * LANES]
                )

        @pl.when(sector == sectors - 1)
        def _():
            @pl.loop(0, count)
            def _(part):
                pltpu.make_async_copy(
                    packed.at[pair, pl.ds(pl.multiple_of(part * rows, SUBLANES), rows)],
                    out_ref.at[part, pair],
                    out_sem,
                ).start()

    pltpu.make_async_copy(out_ref, out_ref, out_sem).wait()


def halve(sizes, operators, basis, count, rows):
    pairs, sectors, height, width = operators.shape
    dtype = operators.dtype
    return pl.pallas_call(
        halve_kernel,
        out_shape=jax.ShapeDtypeStruct((count, pairs, rows, LANES), dtype),
        in_specs=[HBM, HBM, HBM],
        out_specs=HBM,
        scratch_shapes=[
            pltpu.SMEM(sizes.shape, sizes.dtype),
            pltpu.VMEM(operators.shape, dtype),
            pltpu.VMEM(basis.shape, dtype),
            pltpu.VMEM((sectors, width, height), dtype),
            pltpu.VMEM((pairs, count * rows + width, LANES), dtype),
            pltpu.SemaphoreType.DMA,
            pltpu.SemaphoreType.DMA((pairs * sectors,)),
            pltpu.SemaphoreType.DMA((sectors,)),
            pltpu.SemaphoreType.DMA,
        ],
        cost_estimate=pl.CostEstimate(
            flops=2 * operators.size * width,
            bytes_accessed=4 * operators.size,
            transcendentals=0,
        ),
        name="halve",
    )(sizes, operators, basis)


def finish_kernel(
    sizes_hbm, offset_hbm, strips_ref, turned_ref, out_ref,
    sizes_ref, offset_ref, packed, target, half, result,
    size_sem, offset_sem, in_sem, target_sem, out_sem,
):
    pairs, sectors, width = result.shape[0], result.shape[1], result.shape[3]
    count, rows = strips_ref.shape[0], strips_ref.shape[2]
    sizes_copy = pltpu.make_async_copy(sizes_hbm, sizes_ref, size_sem)
    sizes_copy.start()
    offset_copy = pltpu.make_async_copy(offset_hbm, offset_ref, offset_sem)
    offset_copy.start()

    def fetch(pair, sector):
        slot = pair * sectors + sector
        return pltpu.make_async_copy(
            turned_ref.at[sector + 1 + offset_ref[pair]],
            target.at[slot],
            target_sem.at[slot],
        )

    for pair in range(pairs):

        @pl.loop(0, count)
        def _(part):
            pltpu.make_async_copy(
                strips_ref.at[part, pair],
                packed.at[pair, pl.ds(pl.multiple_of(part * rows, SUBLANES), rows)],
                in_sem.at[pair],
            ).start()

        if pair == 0:
            offset_copy.wait()
        for sector in range(sectors):
            fetch(pair, sector).start()

    sizes_copy.wait()
    _, region = regions_of(sizes_ref, sectors, width // LANES)

    @pl.loop(0, pairs * sectors)
    def _(index):
        pair, sector = index // sectors, index % sectors
        start, height = region(sector)

        @pl.when(sector == 0)
        def _():
            whole = packed.at[pair, pl.ds(0, count * rows)]
            pltpu.make_async_copy(whole, whole, in_sem.at[pair]).wait()

        for lane in range(width // LANES):
            half[:, lane * LANES : (lane + 1) * LANES] = packed[
                pair, pl.ds(pl.multiple_of(start + lane * height, STEP), width), :
            ]

        @pl.loop(height // STEP, width // STEP)
        def _(step):
            row = pl.multiple_of(step * STEP, STEP)
            half[pl.ds(row, STEP), :] = jnp.zeros((STEP, width), half.dtype)

        fetch(pair, sector).wait()
        for tile in range(width // TILE):
            span = slice(tile * TILE, (tile + 1) * TILE)
            result[pair, sector, :, span] = times_transposed(
                target[index], half[span, :]
            ).astype(result.dtype)
            pltpu.make_async_copy(
                result.at[pair, sector, :, span], out_ref.at[pair, sector, :, span], out_sem
            ).start()

    pltpu.make_async_copy(out_ref, out_ref, out_sem).wait()


def finish(sizes, offsets, strips, turned, shape):
    pairs, sectors, height, width = shape
    count, _, rows, _ = strips.shape
    dtype = strips.dtype
    size = pairs * sectors * height * width
    return pl.pallas_call(
        finish_kernel,
        out_shape=jax.ShapeDtypeStruct(shape, dtype),
        in_specs=[HBM, HBM, HBM, HBM],
        out_specs=HBM,
        scratch_shapes=[
            pltpu.SMEM(sizes.shape, sizes.dtype),
            pltpu.SMEM(offsets.shape, offsets.dtype),
            pltpu.VMEM((pairs, count * rows + width, LANES), dtype),
            pltpu.VMEM((pairs * sectors, height, width), dtype),
            pltpu.VMEM((width, height), dtype),
            pltpu.VMEM(shape, dtype),
            pltpu.SemaphoreType.DMA,
            pltpu.SemaphoreType.DMA,
            pltpu.SemaphoreType.DMA((pairs,)),
            pltpu.SemaphoreType.DMA((pairs * sectors,)),
            pltpu.SemaphoreType.DMA,
        ],
        cost_estimate=pl.CostEstimate(
            flops=2 * size * width, bytes_accessed=6 * size, transcendentals=0
        ),
        name="finish",
    )(sizes, offsets, strips, turned)


def reorder_kernel(dest_ref, in_ref, out_ref, out_sem):
    @pl.loop(0, in_ref.shape[0], unroll=8)
    def _(pair):
        pltpu.make_async_copy(
            in_ref.at[pair], out_ref.at[dest_ref[pair]], out_sem
        ).start()

    pltpu.make_async_copy(out_ref, out_ref, out_sem).wait()


def reorder(blocks, dest):
    return pl.pallas_call(
        reorder_kernel,
        out_shape=jax.ShapeDtypeStruct(blocks.shape, blocks.dtype),
        in_specs=[SMEM, HBM],
        out_specs=HBM,
        scratch_shapes=[pltpu.SemaphoreType.DMA],
        cost_estimate=pl.CostEstimate(
            flops=0, bytes_accessed=4 * blocks.size, transcendentals=0
        ),
        compiler_params=pltpu.CompilerParams(vmem_limit_bytes=8 << 20),
        name="reorder",
    )(dest, blocks)


def turned_basis(basis, sector_sizes):
    sectors, width = basis.shape[0], basis.shape[2]
    sec_count, sec_pos = lax.axis_size("sec"), lax.axis_index("sec")
    total = sectors * sec_count
    forward = [(i, (i + 1) % sec_count) for i in range(sec_count)]
    backward = [(j, i) for i, j in forward]
    low = lax.ppermute(basis[-1:], "sec", forward)
    high = lax.ppermute(basis[:1], "sec", backward)
    near = jnp.concatenate([low, basis, high], axis=0)
    near_ids = (sec_pos * sectors - 1 + jnp.arange(sectors + 2, dtype=jnp.int32)) % total
    sizes = jnp.sum(
        jnp.where(
            near_ids[:, None] == jnp.arange(total, dtype=jnp.int32)[None, :],
            sector_sizes[None, :],
            0,
        ),
        axis=1,
    )
    kept = jnp.arange(width, dtype=jnp.int32)[None, :] < sizes[:, None]
    return jnp.swapaxes(jnp.where(kept[:, None, :], near, jnp.zeros_like(near)), 1, 2)


def pipeline(rows, operators, basis, shift, dest, sector_sizes):
    pairs = operators.shape[0]
    count = lax.axis_size("ops")
    strips = halve(sector_sizes, operators, basis, count, rows)
    spread = lax.all_to_all(strips, "ops", 0, 0, tiled=True)
    turned = turned_basis(basis, sector_sizes)
    mine = lax.axis_index("ops") * pairs + jnp.arange(pairs, dtype=jnp.int32)
    offsets = jnp.sum(jnp.where(mine[:, None] == dest[None, :], shift[None, :], 0), axis=1)
    spread, turned, offsets = lax.optimization_barrier((spread, turned, offsets))
    ordered = reorder(spread.reshape((count * pairs,) + spread.shape[2:]), dest)
    back = lax.all_to_all(ordered.reshape(spread.shape), "ops", 0, 0, tiled=True)
    return finish(sector_sizes, offsets, back, turned, operators.shape)


def body(operators, basis, shift, dest, sector_sizes):
    sectors, width = operators.shape[1], operators.shape[3]
    lanes, part = width // LANES, lax.axis_size("ops") * SUBLANES
    most = lanes * sectors * width // part
    least = most - CHOICES + 1
    heights = (sector_sizes + STEP - 1) // STEP * STEP
    longest = jnp.max(jnp.sum(heights.reshape(-1, sectors), axis=1)) * lanes
    choice = jnp.clip((longest + part - 1) // part - least, 0, CHOICES - 1)
    return lax.switch(
        choice,
        [
            functools.partial(pipeline, SUBLANES * tiles)
            for tiles in range(least, most + 1)
        ],
        operators, basis, shift, dest, sector_sizes,
    )


def solution(mesh):
    return jax.shard_map(
        body,
        mesh=mesh,
        in_specs=(P("ops", "sec", None, None), P("sec", None, None), P(), P(), P()),
        out_specs=P("ops", "sec", None, None),
        check_vma=False,
    )
```
